32 devices in a mesh: rows: 4 (over y, core), cols: 8 (over z, x).
Axes of the slice: x: 2, y: 2, z: 4, core: 2. Of those that a mesh axis runs over, the one named last changes fastest.
Arguments:
- left_factors: bfloat16 [32, 64, 96, 512], P('rows', 'cols'), may hold values from -0.078125 to 0.078125
- right_factors: bfloat16 [32, 64, 96, 512], P('rows', 'cols'), may hold values from -0.25 to 0.25
- ranks: int32 [32, 64], P('rows', 'cols'), may hold values from 8 to 96
- inputs: bfloat16 [32768, 256], P(('cols', 'rows')), may hold values from -6 to 6
- targets: bfloat16 [16384, 256], P(('rows', 'cols')), may hold values from -6 to 6
Outputs:
- gradient: float32 [32768, 256], P(('cols', 'rows'))
The draws below stay inside these ranges and needn't reach their ends.
All inputs are finite; a program needn't handle non-finite values.
Results may differ from the reference program's by a relative error of at most 0.0073.
Values may be sent and summed in bfloat16 or wider, within the bound.
No kernel may reach another device: no remote copies, remote signals or barrier semaphores. Data moves between devices by JAX's collectives and lax.ppermute only.
A program may use at most 64 MiB of HBM per device.

```python
import jax
import jax.numpy as jnp
from jax import lax

B = 512
RMAX = 96
K = 256
TROWS = 32
TCOLS = 64
NR = 16384
NC = 32768


def touch_ends(values, stream_key, low, high):
    place = [jax.random.randint(jax.random.fold_in(stream_key, axis), (), 0, length) for axis, length in enumerate(values.shape)]
    widest = values.shape.index(max(values.shape))
    next_to = place[:widest] + [(place[widest] + 1) % values.shape[widest]] + place[widest + 1:]
    return values.at[tuple(place)].set(low).at[tuple(next_to)].set(high)


def level_of(stream_key, extent, pieces, least, largest):
    loudness = 1.0
    for dim, shards_of in pieces:
        heights = jax.random.uniform(jax.random.fold_in(jax.random.fold_in(stream_key, 6), dim), (shards_of,), jnp.float32, least / len(pieces), largest / len(pieces))
        loudness = loudness * jnp.repeat(jnp.exp(heights), extent[dim] // shards_of).reshape((-1,) + (1,) * (len(extent) - 1 - dim))
    return loudness


def scatter_about(key, shape, spread, bound, cuts=(), kind=jnp.bfloat16):
    drawn = jax.random.normal(key, shape, jnp.float32) * spread
    if len(cuts) > 0:
        drawn = level_of(key, shape, cuts, -0.22, 0.18) * drawn
    return jnp.clip(drawn, min=-bound, max=bound).astype(kind)


def setup_inputs(seed: int = 0) -> dict:
    seeds = jax.random.split(jax.random.key(seed), 6)
    left_factors = scatter_about(seeds[0], (TROWS, TCOLS, RMAX, B), (RMAX * TCOLS) ** -0.5, 0.078125, ((0, 4), (1, 8)))
    right_factors = scatter_about(seeds[1], (TROWS, TCOLS, RMAX, B), B ** -0.5, 0.25, ((0, 4), (1, 8)))
    ranks = touch_ends(jax.random.randint(seeds[2], (TROWS, TCOLS), RMAX // 12, RMAX + 1), jax.random.fold_in(seeds[2], 1), RMAX // 12, RMAX).astype(jnp.int32)
    inputs = scatter_about(seeds[3], (NC, K), 1.0, 6.0, ((0, 32),))
    targets = scatter_about(seeds[4], (NR, K), 1.0, 6.0, ((0, 32),))
    return {"left_factors": left_factors, "right_factors": right_factors, "ranks": ranks, "inputs": inputs, "targets": targets}


huber_scale = 1.0

def reference(left_factors, right_factors, ranks, inputs, targets):
    input_tiles = inputs.astype(jnp.float32).reshape(TCOLS, B, K)
    target_tiles = targets.astype(jnp.float32).reshape(TROWS, B, K)
    levels = jnp.arange(RMAX, dtype=jnp.int32)

    def tile_row(accumulated, row_data):
        left_row, right_row, rank_row, target = row_data
        active = levels[None, :, None] < rank_row[:, None, None]
        left_wide = left_row.astype(jnp.float32)
        right_wide = right_row.astype(jnp.float32)
        coefficient = jnp.einsum('jrb,jbk->jrk', right_wide, input_tiles)
        coefficient = jnp.where(active, coefficient, 0.0).astype(jnp.bfloat16)
        forward = jnp.einsum('jrb,jrk->bk', left_wide, coefficient.astype(jnp.float32))
        residual = forward - target
        slopes = (residual / jnp.sqrt(1.0 + jnp.square(residual / huber_scale))).astype(jnp.bfloat16)
        adjoint = jnp.einsum('jrb,bk->jrk', left_wide, slopes.astype(jnp.float32))
        adjoint = jnp.where(active, adjoint, 0.0).astype(jnp.bfloat16)
        accumulated = accumulated + jnp.einsum('jrb,jrk->jbk', right_wide, adjoint.astype(jnp.float32))
        return (accumulated, None)
    start = jnp.zeros((TCOLS, B, K), jnp.float32)
    accumulated, _ = lax.scan(tile_row, start, (left_factors, right_factors, ranks, target_tiles))
    return accumulated.reshape(TCOLS * B, K)
```

```python
import jax
import jax.numpy as jnp
from jax import lax
from jax.sharding import PartitionSpec as P

huber_scale = 1.0
CORES = 2


def grid_cycle(count):
    width = 1 << ((count.bit_length() - 1) // 2)
    depth = count // width
    if width % 2 or depth < 2 or depth * width != count:
        return list(range(count))
    places = []
    for x in range(width):
        run = range(1, depth) if x % 2 == 0 else range(depth - 1, 0, -1)
        places += [z * width + x for z in run]
    places += [x for x in range(width - 1, -1, -1)]
    return places


def pseudo_slope(residual):
    return (residual / jnp.sqrt(1.0 + jnp.square(residual / huber_scale))).astype(jnp.bfloat16)


def shards_of(tiles, count):
    number, width, size = tiles.shape
    if count >= number:
        parts = count // number
        cut = tiles.reshape(number, width, parts, size // parts).transpose(0, 2, 1, 3)
        return cut.reshape(count, width, size // parts)
    group = number // count
    cut = tiles.reshape(count, group, width, size).transpose(0, 2, 1, 3)
    return cut.reshape(count, width, group * size)


def tiles_of(shards, number, size):
    count, width, rows = shards.shape
    if count >= number:
        parts = count // number
        cut = shards.reshape(number, parts, width, rows).transpose(0, 2, 1, 3)
        return cut.reshape(number, width, size)
    group = number // count
    cut = shards.reshape(count, width, group, size).transpose(0, 2, 1, 3)
    return cut.reshape(number, width, size)


def solution(mesh):
    row_count, col_count = mesh.shape["rows"], mesh.shape["cols"]
    cores = CORES if row_count % CORES == 0 else 1
    y_count = row_count // cores
    cycle = grid_cycle(col_count)
    place_of = [cycle.index(c) for c in range(col_count)]
    both = ("rows", "cols")

    def ring_pairs():
        pairs = []
        for row in range(row_count):
            step = 1 if row % cores == 0 else -1
            for col in range(col_count):
                target = cycle[(place_of[col] + step) % col_count]
                pairs.append((row * col_count + col, row * col_count + target))
        return pairs

    ring = ring_pairs()
    core_swap = [(r, r - r % cores + (r + 1) % cores) for r in range(row_count)]
    y_next = [(r, (r + cores) % row_count) for r in range(row_count)]
    ring_table = [
        [[cycle[(place_of[col] - step * s) % col_count] for s in range(col_count + 1)] for col in range(col_count)]
        for step in (1, -1)
    ]

    def on_device(left_factors, right_factors, ranks, inputs, targets):
        row_tiles, col_tiles, rank_cap, tile_size = left_factors.shape
        width = inputs.shape[1]
        row, col = lax.axis_index("rows"), lax.axis_index("cols")
        y, core = row // cores, row % cores
        order = jnp.asarray(ring_table, jnp.int32)[core, col]

        mine = inputs
        chip_blocks = [mine]
        for _ in range(y_count - 1):
            mine = lax.ppermute(mine, "rows", y_next)
            chip_blocks.append(mine)
        column_block = jnp.zeros((row_count,) + inputs.shape, inputs.dtype)
        for t, block in enumerate(chip_blocks):
            source = (y - t) % y_count
            column_block = lax.dynamic_update_index_in_dim(column_block, block, source * cores + core, 0)
            if cores > 1:
                other = lax.ppermute(block, "rows", core_swap)
                column_block = lax.dynamic_update_index_in_dim(
                    column_block, other, source * cores + 1 - core, 0
                )
        input_tiles = column_block.reshape(col_tiles, tile_size, width)

        levels = jnp.arange(rank_cap, dtype=jnp.int32)
        active = (levels[None, None, :] < ranks[:, :, None])[..., None]
        coefficient = jnp.einsum(
            "ijrb,jbk->ijrk", right_factors, input_tiles, preferred_element_type=jnp.float32
        )
        coefficient = jnp.where(active, coefficient, 0.0).astype(jnp.bfloat16)
        partial_value = jnp.einsum(
            "ijrb,ijrk->ikb", left_factors, coefficient, preferred_element_type=jnp.float32
        ).astype(jnp.bfloat16)
        shares = shards_of(partial_value, col_count)

        moving = lax.dynamic_index_in_dim(shares, order[1], 0, False)
        for s in range(col_count - 1):
            moving = lax.ppermute(moving, both, ring)
            total = moving.astype(jnp.float32) + lax.dynamic_index_in_dim(
                shares, order[s + 2], 0, False
            ).astype(jnp.float32)
            moving = total.astype(jnp.bfloat16)
        share_slopes = pseudo_slope(total - targets.T.astype(jnp.float32))

        slopes = jnp.zeros((col_count,) + share_slopes.shape, jnp.bfloat16)
        moving = share_slopes
        slopes = lax.dynamic_update_index_in_dim(slopes, moving, col, 0)
        for s in range(col_count - 1):
            moving = lax.ppermute(moving, both, ring)
            slopes = lax.dynamic_update_index_in_dim(slopes, moving, order[s + 1], 0)
        slope_tiles = tiles_of(slopes, row_tiles, tile_size)
        adjoint = jnp.einsum(
            "ijrb,ikb->ijrk", left_factors, slope_tiles, preferred_element_type=jnp.float32
        )
        adjoint = jnp.where(active, adjoint, 0.0).astype(jnp.bfloat16)
        column_terms = jnp.einsum(
            "ijrb,ijrk->jkb", right_factors, adjoint, preferred_element_type=jnp.float32
        ).astype(jnp.bfloat16)
        shares = shards_of(column_terms, row_count)
        shares = shares.reshape((y_count, cores) + shares.shape[1:])

        own = lax.dynamic_index_in_dim(shares, core, 1, False).astype(jnp.float32)
        if cores > 1:
            other = lax.ppermute(lax.dynamic_index_in_dim(shares, 1 - core, 1, False), "rows", core_swap)
            own = own + other.astype(jnp.float32)
        total = lax.dynamic_index_in_dim(own, (y - 1) % y_count, 0, False)
        for s in range(y_count - 1):
            moving = lax.ppermute(total.astype(jnp.bfloat16), "rows", y_next)
            total = moving.astype(jnp.float32) + lax.dynamic_index_in_dim(
                own, (y - 2 - s) % y_count, 0, False
            )
        return total.T

    in_specs = (
        P("rows", "cols", None, None),
        P("rows", "cols", None, None),
        P("rows", "cols"),
        P(("cols", "rows"), None),
        P(("rows", "cols"), None),
    )
    out_specs = P(("cols", "rows"), None)
    return jax.shard_map(
        on_device, mesh=mesh, in_specs=in_specs, out_specs=out_specs, check_vma=False
    )
```

```python
import jax
import jax.numpy as jnp
from jax import lax
from jax.sharding import PartitionSpec as P

huber_scale = 1.0
CORES = 2


def grid_cycle(count):
    width = 1 << ((count.bit_length() - 1) // 2)
    depth = count // width
    if width % 2 or depth < 2 or depth * width != count:
        return list(range(count))
    places = []
    for x in range(width):
        run = range(1, depth) if x % 2 == 0 else range(depth - 1, 0, -1)
        places += [z * width + x for z in run]
    places += [x for x in range(width - 1, -1, -1)]
    return places


def pseudo_slope(residual):
    return (residual / jnp.sqrt(1.0 + jnp.square(residual / huber_scale))).astype(jnp.bfloat16)


def shards_of(tiles, count):
    number, width, size = tiles.shape
    if count >= number:
        parts = count // number
        cut = tiles.reshape(number, width, parts, size // parts).transpose(0, 2, 1, 3)
        return cut.reshape(count, width, size // parts)
    group = number // count
    cut = tiles.reshape(count, group, width, size).transpose(0, 2, 1, 3)
    return cut.reshape(count, width, group * size)


def tiles_of(shards, number, size):
    count, width, rows = shards.shape
    if count >= number:
        parts = count // number
        cut = shards.reshape(number, parts, width, rows).transpose(0, 2, 1, 3)
        return cut.reshape(number, width, size)
    group = number // count
    cut = shards.reshape(count, width, group, size).transpose(0, 2, 1, 3)
    return cut.reshape(number, width, size)


def solution(mesh):
    row_count, col_count = mesh.shape["rows"], mesh.shape["cols"]
    cores = CORES if row_count % CORES == 0 else 1
    y_count = row_count // cores
    half_way = col_count // 2
    cycle = grid_cycle(col_count)
    place_of = [cycle.index(c) for c in range(col_count)]
    ahead = [(cycle[p], cycle[(p + 1) % col_count]) for p in range(col_count)]
    behind = [(b, a) for a, b in ahead]
    core_swap = [(r, r - r % cores + (r + 1) % cores) for r in range(row_count)]
    y_next = [(r, (r + cores) % row_count) for r in range(row_count)]
    place_table = [
        [cycle[(place_of[col] + d) % col_count] for d in range(col_count)] for col in range(col_count)
    ]

    def on_device(left_factors, right_factors, ranks, inputs, targets):
        row_tiles, col_tiles, rank_cap, tile_size = left_factors.shape
        width = inputs.shape[1]
        row, col = lax.axis_index("rows"), lax.axis_index("cols")
        y, core = row // cores, row % cores
        at = jnp.asarray(place_table, jnp.int32)[col]
        one_tile = col_count == row_tiles
        wide = lambda block: block.astype(jnp.float32)
        narrow = lambda block: block.astype(jnp.bfloat16)
        pick = lambda array, index, dim=0: lax.dynamic_index_in_dim(array, index, dim, False)

        levels = jnp.arange(rank_cap, dtype=jnp.int32)
        active = levels[None, None, :] < ranks[:, :, None]

        group = col_tiles // row_count

        def coefficients_of(block, source, buffer):
            first = source * group
            factors = lax.dynamic_slice_in_dim(right_factors, first, group, 1)
            mask = lax.dynamic_slice_in_dim(active, first, group, 1)
            product = jnp.einsum(
                "ijrb,jbk->jirk",
                factors,
                block.reshape(group, tile_size, width),
                preferred_element_type=jnp.float32,
            )
            product = narrow(jnp.where(mask.transpose(1, 0, 2)[..., None], product, 0.0))
            return lax.dynamic_update_slice_in_dim(buffer, product, first, 0)

        coefficient = jnp.zeros((col_tiles, row_tiles, rank_cap, width), jnp.bfloat16)
        mine = inputs
        for t in range(y_count):
            source = (y - t) % y_count
            following = lax.ppermute(mine, "rows", y_next) if t + 1 < y_count else None
            if cores > 1:
                other = lax.ppermute(mine, "rows", core_swap)
            coefficient = coefficients_of(mine, source * cores + core, coefficient)
            if cores > 1:
                coefficient = coefficients_of(other, source * cores + 1 - core, coefficient)
            mine = following

        if one_tile:

            def part(d):
                tile = jnp.einsum(
                    "jrk,jrb->kb",
                    pick(coefficient, at[d], 1),
                    pick(left_factors, at[d]),
                    preferred_element_type=jnp.float32,
                )
                return lax.optimization_barrier(narrow(tile))

        else:
            shares = jnp.einsum(
                "ijrb,jirk->ikb", left_factors, coefficient, preferred_element_type=jnp.float32
            )
            shares = shards_of(narrow(shares), col_count)

            def part(d):
                return pick(shares, at[d])

        cut = width // 2
        far = part(half_way)
        up, down = far[:cut], far[cut:]
        for d in range(half_way - 1, -1, -1):
            up = lax.ppermute(up, "cols", ahead)
            down = lax.ppermute(down, "cols", behind)
            own_up = part(d)
            own_down = part(col_count - d) if d else None
            if up.shape[0] == cut:
                up = jnp.concatenate([wide(up), jnp.zeros(up.shape, jnp.float32)])
                down = jnp.concatenate([jnp.zeros(down.shape, jnp.float32), wide(down)])
            if d:
                up = narrow(wide(up) + wide(own_up))
                down = narrow(wide(down) + wide(own_down))
            else:
                total = wide(own_up) + wide(up) + wide(down)
        share_slopes = pseudo_slope(total - targets.T.astype(jnp.float32))

        if one_tile:

            def adjoint_of(block, d, buffer):
                product = jnp.einsum(
                    "jrb,kb->jrk", pick(left_factors, at[d]), block, preferred_element_type=jnp.float32
                )
                product = narrow(jnp.where(pick(active, at[d])[..., None], product, 0.0))
                return lax.dynamic_update_index_in_dim(buffer, product, at[d], 0)

            gathered = jnp.zeros((row_tiles, col_tiles, rank_cap, width), jnp.bfloat16)
        else:

            def adjoint_of(block, d, buffer):
                return lax.dynamic_update_index_in_dim(buffer, block, at[d], 0)

            gathered = jnp.zeros((col_count,) + share_slopes.shape, jnp.bfloat16)
        up = down = share_slopes
        held, places = [share_slopes], [0]
        for d in range(1, half_way + 1):
            if d == half_way:
                up, down = up[:cut], down[cut:]
            up = lax.ppermute(up, "cols", ahead)
            down = lax.ppermute(down, "cols", behind)
            for block, place in zip(held, places):
                gathered = adjoint_of(block, place, gathered)
            if d == half_way:
                held, places = [jnp.concatenate([up, down])], [half_way]
            else:
                held, places = [up, down], [col_count - d, d]
        for block, place in zip(held, places):
            gathered = adjoint_of(block, place, gathered)
        adjoint = gathered
        if not one_tile:
            adjoint = jnp.einsum(
                "ijrb,ikb->ijrk",
                left_factors,
                tiles_of(gathered, row_tiles, tile_size),
                preferred_element_type=jnp.float32,
            )
            adjoint = narrow(jnp.where(active[..., None], adjoint, 0.0))
        column_terms = narrow(
            jnp.einsum("ijrb,ijrk->jkb", right_factors, adjoint, preferred_element_type=jnp.float32)
        )
        shares = column_terms.reshape((y_count, cores, group) + column_terms.shape[1:])

        own = pick(shares, core, 1)
        if cores > 1:
            other = lax.ppermute(pick(shares, 1 - core, 1), "rows", core_swap)
            own = wide(own) + wide(other)
        total = pick(own, (y - 1) % y_count)
        for s in range(y_count - 1):
            moving = lax.ppermute(narrow(total), "rows", y_next)
            total = wide(moving) + wide(pick(own, (y - 2 - s) % y_count))
        return total.transpose(0, 2, 1).reshape(group * tile_size, width)

    in_specs = (
        P("rows", "cols", None, None),
        P("rows", "cols", None, None),
        P("rows", "cols"),
        P(("cols", "rows"), None),
        P(("rows", "cols"), None),
    )
    out_specs = P(("cols", "rows"), None)
    return jax.shard_map(
        on_device, mesh=mesh, in_specs=in_specs, out_specs=out_specs, check_vma=False
    )
```

```python
import jax
import jax.numpy as jnp
from jax import lax
from jax.sharding import PartitionSpec as P

huber_scale = 1.0
CORES = 2


def grid_cycle(count):
    width = 1 << ((count.bit_length() - 1) // 2)
    depth = count // width
    if width % 2 or depth < 2 or depth * width != count:
        return list(range(count))
    places = []
    for x in range(width):
        run = range(1, depth) if x % 2 == 0 else range(depth - 1, 0, -1)
        places += [z * width + x for z in run]
    places += [x for x in range(width - 1, -1, -1)]
    return places


def pseudo_slope(residual):
    return (residual / jnp.sqrt(1.0 + jnp.square(residual / huber_scale))).astype(jnp.bfloat16)


def shards_of(tiles, count):
    number, width, size = tiles.shape
    if count >= number:
        parts = count // number
        cut = tiles.reshape(number, width, parts, size // parts).transpose(0, 2, 1, 3)
        return cut.reshape(count, width, size // parts)
    group = number // count
    cut = tiles.reshape(count, group, width, size).transpose(0, 2, 1, 3)
    return cut.reshape(count, width, group * size)


def tiles_of(shards, number, size):
    count, width, rows = shards.shape
    if count >= number:
        parts = count // number
        cut = shards.reshape(number, parts, width, rows).transpose(0, 2, 1, 3)
        return cut.reshape(number, width, size)
    group = number // count
    cut = shards.reshape(count, width, group, size).transpose(0, 2, 1, 3)
    return cut.reshape(number, width, size)


def solution(mesh):
    row_count, col_count = mesh.shape["rows"], mesh.shape["cols"]
    cores = CORES if row_count % CORES == 0 else 1
    y_count = row_count // cores
    half_way = col_count // 2
    cycle = grid_cycle(col_count)
    place_of = [cycle.index(c) for c in range(col_count)]
    ahead = [(cycle[p], cycle[(p + 1) % col_count]) for p in range(col_count)]
    behind = [(b, a) for a, b in ahead]
    core_swap = [(r, r - r % cores + (r + 1) % cores) for r in range(row_count)]
    y_next = [(r, (r + cores) % row_count) for r in range(row_count)]

    def indices_of(row, col, group):
        y, core = row // cores, row % cores
        found = [cycle[(place_of[col] + d) % col_count] for d in range(col_count)]
        for t in range(y_count):
            source = ((y - t) % y_count) * cores
            for c in range(cores):
                found.append((source + (core + c) % cores) * group)
        return found

    def on_device(left_factors, right_factors, ranks, inputs, targets):
        row_tiles, col_tiles, rank_cap, tile_size = left_factors.shape
        width = inputs.shape[1]
        group = col_tiles // row_count
        table = [[indices_of(r, c, group) for c in range(col_count)] for r in range(row_count)]
        table = jnp.asarray(table, jnp.int32)
        here = lax.dynamic_slice(
            table,
            (lax.axis_index("rows"), lax.axis_index("cols"), 0),
            (1, 1, table.shape[2]),
            allow_negative_indices=False,
        )[0, 0]
        at = [here[d] for d in range(col_count)]
        first_tile = [
            [here[col_count + t * cores + c] for c in range(cores)] for t in range(y_count)
        ]
        one_tile = col_count == row_tiles
        wide = lambda block: block.astype(jnp.float32)
        narrow = lambda block: block.astype(jnp.bfloat16)
        window = lambda array, index, size, dim=0: lax.dynamic_slice_in_dim(
            array, index, size, dim, allow_negative_indices=False
        )
        pick = lambda array, index, dim=0: lax.squeeze(window(array, index, 1, dim), (dim,))
        put = lambda array, piece, index: lax.dynamic_update_slice_in_dim(
            array, piece, index, 0, allow_negative_indices=False
        )

        levels = jnp.arange(rank_cap, dtype=jnp.int32)
        active = levels[None, None, :] < ranks[:, :, None]

        def coefficients_of(block, first, buffer):
            count = block.shape[0] // tile_size
            product = jnp.einsum(
                "ijrb,jbk->jirk",
                window(right_factors, first, count, 1),
                block.reshape(count, tile_size, width),
                preferred_element_type=jnp.float32,
            )
            mask = window(active, first, count, 1).transpose(1, 0, 2)
            product = narrow(jnp.where(mask[..., None], product, 0.0))
            return put(buffer, product, first)

        coefficient = jnp.zeros((col_tiles, row_tiles, rank_cap, width), jnp.bfloat16)
        mine = inputs
        for t in range(y_count):
            if t + 1 < y_count:
                following = lax.ppermute(mine, "rows", y_next)
            others = [mine]
            for _ in range(cores - 1):
                others.append(lax.ppermute(others[-1], "rows", core_swap))
            for c, other in enumerate(others):
                coefficient = coefficients_of(other, first_tile[t][c], coefficient)
            mine = following

        if one_tile:

            def part(d):
                tile = jnp.einsum(
                    "jrk,jrb->kb",
                    pick(coefficient, at[d], 1),
                    pick(left_factors, at[d]),
                    preferred_element_type=jnp.float32,
                )
                return lax.optimization_barrier(narrow(tile))

        else:
            shares = jnp.einsum(
                "ijrb,jirk->ikb", left_factors, coefficient, preferred_element_type=jnp.float32
            )
            shares = shards_of(narrow(shares), col_count)

            def part(d):
                return pick(shares, at[d])

        cut = width // 2
        far = part(half_way)
        up, down = far[:cut], far[cut:]
        for d in range(half_way - 1, -1, -1):
            up = lax.ppermute(up, "cols", ahead)
            down = lax.ppermute(down, "cols", behind)
            own_up = part(d)
            own_down = part(col_count - d) if d else None
            if up.shape[0] == cut:
                up = jnp.concatenate([wide(up), jnp.zeros(up.shape, jnp.float32)])
                down = jnp.concatenate([jnp.zeros(down.shape, jnp.float32), wide(down)])
            if d:
                up = narrow(wide(up) + wide(own_up))
                down = narrow(wide(down) + wide(own_down))
            else:
                total = wide(own_up) + wide(up) + wide(down)
        share_slopes = pseudo_slope(total - targets.T.astype(jnp.float32))

        if one_tile:

            def adjoint_of(block, d, buffer):
                product = jnp.einsum(
                    "jrb,kb->jrk", pick(left_factors, at[d]), block, preferred_element_type=jnp.float32
                )
                product = narrow(jnp.where(pick(active, at[d])[..., None], product, 0.0))
                return put(buffer, product[None], at[d])

            gathered = jnp.zeros((row_tiles, col_tiles, rank_cap, width), jnp.bfloat16)
        else:

            def adjoint_of(block, d, buffer):
                return put(buffer, block[None], at[d])

            gathered = jnp.zeros((col_count,) + share_slopes.shape, jnp.bfloat16)
        up = down = share_slopes
        held, places = [share_slopes], [0]
        for d in range(1, half_way + 1):
            if d == half_way:
                up, down = up[:cut], down[cut:]
            up = lax.ppermute(up, "cols", ahead)
            down = lax.ppermute(down, "cols", behind)
            for block, place in zip(held, places):
                gathered = adjoint_of(block, place, gathered)
            if d == half_way:
                held, places = [jnp.concatenate([up, down])], [half_way]
            else:
                held, places = [up, down], [col_count - d, d]
        for block, place in zip(held, places):
            gathered = adjoint_of(block, place, gathered)
        adjoint = gathered
        if not one_tile:
            adjoint = jnp.einsum(
                "ijrb,ikb->ijrk",
                left_factors,
                tiles_of(gathered, row_tiles, tile_size),
                preferred_element_type=jnp.float32,
            )
            adjoint = narrow(jnp.where(active[..., None], adjoint, 0.0))

        def terms(factors, values, t, c):
            first = first_tile[t % y_count][c]
            product = jnp.einsum(
                "ijrb,ijrk->jkb",
                window(factors, first, group, 1),
                window(values, first, group, 1),
                preferred_element_type=jnp.float32,
            )
            return lax.optimization_barrier(narrow(product))

        def chip_terms(factors, values, t):
            total = wide(terms(factors, values, t, 0))
            if cores > 1:
                other = terms(factors, values, t, 1)
                total = total + wide(lax.ppermute(other, "rows", core_swap))
            return total.transpose(0, 2, 1).reshape(group * tile_size, width)

        factors, values = lax.optimization_barrier((right_factors, adjoint))
        total = chip_terms(factors, values, 1)
        for t in range(2, y_count + 1):
            leaving, factors, values = lax.optimization_barrier((narrow(total), factors, values))
            moving = lax.ppermute(leaving, "rows", y_next)
            total = wide(moving) + lax.optimization_barrier(chip_terms(factors, values, t))
        return total

    in_specs = (
        P("rows", "cols", None, None),
        P("rows", "cols", None, None),
        P("rows", "cols"),
        P(("cols", "rows"), None),
        P(("rows", "cols"), None),
    )
    out_specs = P(("cols", "rows"), None)
    return jax.shard_map(
        on_device, mesh=mesh, in_specs=in_specs, out_specs=out_specs, check_vma=False
    )
```

```python
import jax
import jax.numpy as jnp
import numpy as np
from jax import lax
from jax.sharding import PartitionSpec as P


huber_scale = 1.0
CORES = 2


def grid_cycle(count):
    width = 1 << ((count.bit_length() - 1) // 2)
    depth = count // width
    if width % 2 or depth < 2 or depth * width != count:
        return list(range(count))
    places = []
    for x in range(width):
        run = range(1, depth) if x % 2 == 0 else range(depth - 1, 0, -1)
        places += [z * width + x for z in run]
    places += [x for x in range(width - 1, -1, -1)]
    return places


def pseudo_slope(residual):
    return (residual / jnp.sqrt(1.0 + jnp.square(residual / huber_scale))).astype(jnp.bfloat16)


def shards_of(tiles, count):
    number, width, size = tiles.shape
    if count >= number:
        parts = count // number
        cut = tiles.reshape(number, width, parts, size // parts).transpose(0, 2, 1, 3)
        return cut.reshape(count, width, size // parts)
    group = number // count
    cut = tiles.reshape(count, group, width, size).transpose(0, 2, 1, 3)
    return cut.reshape(count, width, group * size)


def tiles_of(shards, number, size):
    count, width, rows = shards.shape
    if count >= number:
        parts = count // number
        cut = shards.reshape(number, parts, width, rows).transpose(0, 2, 1, 3)
        return cut.reshape(number, width, size)
    group = number // count
    cut = shards.reshape(count, width, group, size).transpose(0, 2, 1, 3)
    return cut.reshape(number, width, size)


def solution(mesh):
    row_count, col_count = mesh.shape["rows"], mesh.shape["cols"]
    cores = CORES if row_count % CORES == 0 else 1
    y_count = row_count // cores
    half_way = col_count // 2
    cycle = grid_cycle(col_count)
    place_of = [cycle.index(c) for c in range(col_count)]
    ahead = [(cycle[p], cycle[(p + 1) % col_count]) for p in range(col_count)]
    behind = [(b, a) for a, b in ahead]
    core_swap = [(r, r - r % cores + (r + 1) % cores) for r in range(row_count)]
    y_next = [(r, (r + cores) % row_count) for r in range(row_count)]

    bits = 32 // col_count if col_count & (col_count - 1) == 0 else 0
    packed = bits > 0 and (1 << bits) >= col_count
    cycle_word = place_word = 0
    if packed:
        cycle_word = int(np.uint32(sum(c << (bits * p) for p, c in enumerate(cycle))).view(np.int32))
        place_word = int(np.uint32(sum(p << (bits * c) for c, p in enumerate(place_of))).view(np.int32))

    def columns_ahead(col):
        if not packed:
            table = [[cycle[(p + d) % col_count] for d in range(col_count)] for p in place_of]
            row = lax.dynamic_index_in_dim(jnp.asarray(table, jnp.int32), col, 0, False)
            return [row[d] for d in range(col_count)]
        low = (1 << bits) - 1
        shift = ((place_word_at(col)) & low) * bits
        word = lax.shift_right_logical(jnp.int32(cycle_word), shift) | (
            (jnp.int32(cycle_word) << (32 - bits - shift)) << bits
        )
        return [lax.shift_right_logical(word, jnp.int32(bits * d)) & low for d in range(col_count)]

    def place_word_at(col):
        return lax.shift_right_logical(jnp.int32(place_word), col * bits)

    def rows_back(row):
        if cores != 2 or row_count & (row_count - 1):
            y, core = row // cores, row % cores
            return [
                [((y - t) % y_count) * cores + (core + c) % cores for c in range(cores)]
                for t in range(y_count)
            ]
        back = [(row + (row_count - t * cores)) & (row_count - 1) if t else row for t in range(y_count)]
        return [[r, r ^ 1] for r in back]

    def on_device(left_factors, right_factors, ranks, inputs, targets):
        row_tiles, col_tiles, rank_cap, tile_size = left_factors.shape
        width = inputs.shape[1]
        group = col_tiles // row_count
        at = columns_ahead(lax.axis_index("cols"))
        first_tile = [[r * group for r in rows] for rows in rows_back(lax.axis_index("rows"))]
        one_tile = col_count == row_tiles
        wide = lambda block: block.astype(jnp.float32)
        narrow = lambda block: block.astype(jnp.bfloat16)
        window = lambda array, index, size, dim=0: lax.dynamic_slice_in_dim(
            array, index, size, dim, allow_negative_indices=False
        )
        pick = lambda array, index, dim=0: lax.squeeze(window(array, index, 1, dim), (dim,))
        put = lambda array, piece, index: lax.dynamic_update_slice_in_dim(
            array, piece, index, 0, allow_negative_indices=False
        )

        levels = jnp.arange(rank_cap, dtype=jnp.int32)
        active = levels[None, None, :] < ranks[:, :, None]

        def coefficients_of(factors, block, first, buffer):
            count = block.shape[0] // tile_size
            product = jnp.einsum(
                "ijrb,jbk->jirk",
                window(factors, first, count, 1),
                block.reshape(count, tile_size, width),
                preferred_element_type=jnp.float32,
            )
            mask = window(active, first, count, 1).transpose(1, 0, 2)
            product = narrow(jnp.where(mask[..., None], product, 0.0))
            return put(buffer, product, first)

        coefficient = jnp.zeros((col_tiles, row_tiles, rank_cap, width), jnp.bfloat16)
        mine = inputs
        for t in range(y_count):
            if t + 1 < y_count:
                following = lax.ppermute(mine, "rows", y_next)
            others = [mine]
            for _ in range(cores - 1):
                others.append(lax.ppermute(others[-1], "rows", core_swap))
            for c, other in enumerate(others):
                factors, other = lax.optimization_barrier((right_factors, other))
                coefficient = coefficients_of(factors, other, first_tile[t][c], coefficient)
            mine = following

        if one_tile:

            def part(d):
                tile = jnp.einsum(
                    "jrk,jrb->kb",
                    pick(coefficient, at[d], 1),
                    pick(left_factors, at[d]),
                    preferred_element_type=jnp.float32,
                )
                return lax.optimization_barrier(narrow(tile))

        else:
            shares = jnp.einsum(
                "ijrb,jirk->ikb", left_factors, coefficient, preferred_element_type=jnp.float32
            )
            shares = shards_of(narrow(shares), col_count)

            def part(d):
                return pick(shares, at[d])

        cut = width // 2
        far = part(half_way)
        up, down = far[:cut], far[cut:]
        for d in range(half_way - 1, -1, -1):
            up = lax.ppermute(up, "cols", ahead)
            down = lax.ppermute(down, "cols", behind)
            own_up = part(d)
            own_down = part(col_count - d) if d else None
            if up.shape[0] == cut:
                up = jnp.concatenate([wide(up), jnp.zeros(up.shape, jnp.float32)])
                down = jnp.concatenate([jnp.zeros(down.shape, jnp.float32), wide(down)])
            if d:
                up = narrow(wide(up) + wide(own_up))
                down = narrow(wide(down) + wide(own_down))
            else:
                total = wide(own_up) + wide(up) + wide(down)
        share_slopes = pseudo_slope(total - targets.T.astype(jnp.float32))

        if one_tile:

            def adjoint_of(block, d, buffer):
                product = jnp.einsum(
                    "jrb,kb->jrk", pick(left_factors, at[d]), block, preferred_element_type=jnp.float32
                )
                product = narrow(jnp.where(pick(active, at[d])[..., None], product, 0.0))
                return put(buffer, product[None], at[d])

            gathered = jnp.zeros((row_tiles, col_tiles, rank_cap, width), jnp.bfloat16)
        else:

            def adjoint_of(block, d, buffer):
                return put(buffer, block[None], at[d])

            gathered = jnp.zeros((col_count,) + share_slopes.shape, jnp.bfloat16)
        up = down = share_slopes
        held, places = [share_slopes], [0]
        for d in range(1, half_way + 1):
            if d == half_way:
                up, down = up[:cut], down[cut:]
            up = lax.ppermute(up, "cols", ahead)
            down = lax.ppermute(down, "cols", behind)
            for block, place in zip(held, places):
                gathered = adjoint_of(block, place, gathered)
            if d == half_way:
                held, places = [jnp.concatenate([up, down])], [half_way]
            else:
                held, places = [up, down], [col_count - d, d]
        for block, place in zip(held, places):
            gathered = adjoint_of(block, place, gathered)
        adjoint = gathered
        if not one_tile:
            adjoint = jnp.einsum(
                "ijrb,ikb->ijrk",
                left_factors,
                tiles_of(gathered, row_tiles, tile_size),
                preferred_element_type=jnp.float32,
            )
            adjoint = narrow(jnp.where(active[..., None], adjoint, 0.0))

        def terms(factors, values, t, c):
            first = first_tile[t % y_count][c]
            product = jnp.einsum(
                "ijrb,ijrk->jkb",
                window(factors, first, group, 1),
                window(values, first, group, 1),
                preferred_element_type=jnp.float32,
            )
            return lax.optimization_barrier(narrow(product))

        def chip_terms(factors, values, t):
            total = wide(terms(factors, values, t, 0))
            if cores > 1:
                other = terms(factors, values, t, 1)
                total = total + wide(lax.ppermute(other, "rows", core_swap))
            return total

        factors, values = lax.optimization_barrier((right_factors, adjoint))
        total = chip_terms(factors, values, 1)
        for t in range(2, y_count + 1):
            leaving, factors, values = lax.optimization_barrier((narrow(total), factors, values))
            moving = lax.ppermute(leaving, "rows", y_next)
            own = lax.optimization_barrier(chip_terms(factors, values, t))
            total = wide(moving) + own
        return total.transpose(0, 2, 1).reshape(group * tile_size, width)

    in_specs = (
        P("rows", "cols", None, None),
        P("rows", "cols", None, None),
        P("rows", "cols"),
        P(("cols", "rows"), None),
        P(("rows", "cols"), None),
    )
    out_specs = P(("cols", "rows"), None)
    return jax.shard_map(
        on_device, mesh=mesh, in_specs=in_specs, out_specs=out_specs, check_vma=False
    )
```

```python
import jax
import jax.numpy as jnp
import numpy as np
from jax import lax
from jax.experimental import pallas as pl
from jax.experimental.pallas import tpu as pltpu
from jax.sharding import PartitionSpec as P


huber_scale = 1.0
CORES = 2


def grid_cycle(count):
    width = 1 << ((count.bit_length() - 1) // 2)
    depth = count // width
    if width % 2 or depth < 2 or depth * width != count:
        return list(range(count))
    places = []
    for x in range(width):
        run = range(1, depth) if x % 2 == 0 else range(depth - 1, 0, -1)
        places += [z * width + x for z in run]
    places += [x for x in range(width - 1, -1, -1)]
    return places


def pseudo_slope(residual):
    return (residual / jnp.sqrt(1.0 + jnp.square(residual / huber_scale))).astype(jnp.bfloat16)


def turned(block):
    def turn(source, target):
        target[...] = source[...].T

    rows, width = block.shape
    return pl.pallas_call(
        turn,
        out_shape=jax.ShapeDtypeStruct((width, rows), block.dtype),
        compiler_params=pltpu.CompilerParams(vmem_limit_bytes=4 << 20),
        name="turned",
    )(block)


def shards_of(tiles, count):
    number, width, size = tiles.shape
    if count >= number:
        parts = count // number
        cut = tiles.reshape(number, width, parts, size // parts).transpose(0, 2, 1, 3)
        return cut.reshape(count, width, size // parts)
    group = number // count
    cut = tiles.reshape(count, group, width, size).transpose(0, 2, 1, 3)
    return cut.reshape(count, width, group * size)


def tiles_of(shards, number, size):
    count, width, rows = shards.shape
    if count >= number:
        parts = count // number
        cut = shards.reshape(number, parts, width, rows).transpose(0, 2, 1, 3)
        return cut.reshape(number, width, size)
    group = number // count
    cut = shards.reshape(count, width, group, size).transpose(0, 2, 1, 3)
    return cut.reshape(number, width, size)


def solution(mesh):
    row_count, col_count = mesh.shape["rows"], mesh.shape["cols"]
    cores = CORES if row_count % CORES == 0 else 1
    y_count = row_count // cores
    half_way = col_count // 2
    cycle = grid_cycle(col_count)
    place_of = [cycle.index(c) for c in range(col_count)]
    ahead = [(cycle[p], cycle[(p + 1) % col_count]) for p in range(col_count)]
    behind = [(b, a) for a, b in ahead]
    core_swap = [(r, r - r % cores + (r + 1) % cores) for r in range(row_count)]
    y_next = [(r, (r + cores) % row_count) for r in range(row_count)]

    bits = 32 // col_count if col_count & (col_count - 1) == 0 else 0
    packed = bits > 0 and (1 << bits) >= col_count
    cycle_word = place_word = 0
    if packed:
        cycle_word = int(np.uint32(sum(c << (bits * p) for p, c in enumerate(cycle))).view(np.int32))
        place_word = int(np.uint32(sum(p << (bits * c) for c, p in enumerate(place_of))).view(np.int32))

    def columns_ahead(col):
        if not packed:
            table = [[cycle[(p + d) % col_count] for d in range(col_count)] for p in place_of]
            row = lax.dynamic_index_in_dim(jnp.asarray(table, jnp.int32), col, 0, False)
            return [row[d] for d in range(col_count)]
        low = (1 << bits) - 1
        shift = ((place_word_at(col)) & low) * bits
        word = lax.shift_right_logical(jnp.int32(cycle_word), shift) | (
            (jnp.int32(cycle_word) << (32 - bits - shift)) << bits
        )
        return [col] + [
            lax.shift_right_logical(word, jnp.int32(bits * d)) & low for d in range(1, col_count)
        ]

    def place_word_at(col):
        return lax.shift_right_logical(jnp.int32(place_word), col * bits)

    def rows_back(row):
        if cores != 2 or row_count & (row_count - 1):
            y, core = row // cores, row % cores
            return [
                [((y - t) % y_count) * cores + (core + c) % cores for c in range(cores)]
                for t in range(y_count)
            ]
        back = [(row + (row_count - t * cores)) & (row_count - 1) if t else row for t in range(y_count)]
        return [[r, r ^ 1] for r in back]

    def on_device(left_factors, right_factors, ranks, inputs, targets):
        row_tiles, col_tiles, rank_cap, tile_size = left_factors.shape
        width = inputs.shape[1]
        group = col_tiles // row_count
        at = columns_ahead(lax.axis_index("cols"))
        first_tile = [[r * group for r in rows] for rows in rows_back(lax.axis_index("rows"))]
        one_tile = col_count == row_tiles
        wide = lambda block: block.astype(jnp.float32)
        narrow = lambda block: block.astype(jnp.bfloat16)
        window = lambda array, index, size, dim=0: lax.dynamic_slice_in_dim(
            array, index, size, dim, allow_negative_indices=False
        )
        pick = lambda array, index, dim=0: lax.squeeze(window(array, index, 1, dim), (dim,))
        put = lambda array, piece, index: lax.dynamic_update_slice_in_dim(
            array, piece, index, 0, allow_negative_indices=False
        )

        goal = turned(targets)

        levels = jnp.arange(rank_cap, dtype=jnp.int32)
        active = levels[None, None, :] < ranks[:, :, None]

        def coefficients_of(factors, block, first, buffer):
            count = block.shape[0] // tile_size
            product = jnp.einsum(
                "ijrb,jbk->jirk",
                window(factors, first, count, 1),
                block.reshape(count, tile_size, width),
                preferred_element_type=jnp.float32,
            )
            mask = window(active, first, count, 1).transpose(1, 0, 2)
            product = narrow(jnp.where(mask[..., None], product, 0.0))
            return put(buffer, product, first)

        coefficient = jnp.zeros((col_tiles, row_tiles, rank_cap, width), jnp.bfloat16)
        mine = inputs
        for t in range(y_count):
            if t + 1 < y_count:
                following = lax.ppermute(mine, "rows", y_next)
            others = [mine]
            for _ in range(cores - 1):
                others.append(lax.ppermute(others[-1], "rows", core_swap))
            for c, other in enumerate(others):
                factors, other = lax.optimization_barrier((right_factors, other))
                coefficient = coefficients_of(factors, other, first_tile[t][c], coefficient)
            mine = following

        if one_tile:

            def part(d):
                tile = jnp.einsum(
                    "jrk,jrb->kb",
                    pick(coefficient, at[d], 1),
                    pick(left_factors, at[d]),
                    preferred_element_type=jnp.float32,
                )
                return lax.optimization_barrier(narrow(tile))

        else:
            shares = jnp.einsum(
                "ijrb,jirk->ikb", left_factors, coefficient, preferred_element_type=jnp.float32
            )
            shares = shards_of(narrow(shares), col_count)

            def part(d):
                return pick(shares, at[d])

        cut = width // 2
        far = part(half_way)
        up, down = far[:cut], far[cut:]
        for d in range(half_way - 1, -1, -1):
            up = lax.ppermute(up, "cols", ahead)
            down = lax.ppermute(down, "cols", behind)
            own_up = part(d)
            own_down = part(col_count - d) if d else None
            if up.shape[0] == cut:
                up = jnp.concatenate([wide(up), jnp.zeros(up.shape, jnp.float32)])
                down = jnp.concatenate([jnp.zeros(down.shape, jnp.float32), wide(down)])
            if d:
                up = narrow(wide(up) + wide(own_up))
                down = narrow(wide(down) + wide(own_down))
            else:
                total = wide(own_up) + wide(up) + wide(down)
        share_slopes = pseudo_slope(total - wide(goal))

        if one_tile:

            def adjoint_of(block, d, buffer):
                product = jnp.einsum(
                    "jrb,kb->jrk", pick(left_factors, at[d]), block, preferred_element_type=jnp.float32
                )
                product = narrow(jnp.where(pick(active, at[d])[..., None], product, 0.0))
                return put(buffer, product[None], at[d])

            gathered = jnp.zeros((row_tiles, col_tiles, rank_cap, width), jnp.bfloat16)
        else:

            def adjoint_of(block, d, buffer):
                return put(buffer, block[None], at[d])

            gathered = jnp.zeros((col_count,) + share_slopes.shape, jnp.bfloat16)
        up = down = share_slopes
        held, places = [share_slopes], [0]
        for d in range(1, half_way + 1):
            if d == half_way:
                up, down = up[:cut], down[cut:]
            up = lax.ppermute(up, "cols", ahead)
            down = lax.ppermute(down, "cols", behind)
            for block, place in zip(held, places):
                gathered = adjoint_of(block, place, gathered)
            if d == half_way:
                held, places = [jnp.concatenate([up, down])], [half_way]
            else:
                held, places = [up, down], [col_count - d, d]
        for block, place in zip(held, places):
            gathered = adjoint_of(block, place, gathered)
        adjoint = gathered
        if not one_tile:
            adjoint = jnp.einsum(
                "ijrb,ikb->ijrk",
                left_factors,
                tiles_of(gathered, row_tiles, tile_size),
                preferred_element_type=jnp.float32,
            )
            adjoint = narrow(jnp.where(active[..., None], adjoint, 0.0))

        def terms(factors, values, t, c):
            first = first_tile[t % y_count][c]
            product = jnp.einsum(
                "ijrb,ijrk->jkb",
                window(factors, first, group, 1),
                window(values, first, group, 1),
                preferred_element_type=jnp.float32,
            )
            return lax.optimization_barrier(narrow(product))

        def chip_terms(factors, values, t):
            total = wide(terms(factors, values, t, 0))
            if cores > 1:
                other = terms(factors, values, t, 1)
                total = total + wide(lax.ppermute(other, "rows", core_swap))
            return total

        factors, values = lax.optimization_barrier((right_factors, adjoint))
        total = chip_terms(factors, values, 1)
        for t in range(2, y_count + 1):
            leaving, factors, values = lax.optimization_barrier((narrow(total), factors, values))
            moving = lax.ppermute(leaving, "rows", y_next)
            own = lax.optimization_barrier(chip_terms(factors, values, t))
            total = wide(moving) + own
        return total.transpose(0, 2, 1).reshape(group * tile_size, width)

    in_specs = (
        P("rows", "cols", None, None),
        P("rows", "cols", None, None),
        P("rows", "cols"),
        P(("cols", "rows"), None),
        P(("rows", "cols"), None),
    )
    out_specs = P(("cols", "rows"), None)
    return jax.shard_map(
        on_device, mesh=mesh, in_specs=in_specs, out_specs=out_specs, check_vma=False
    )
```
